32 devices in a mesh: tm: 8 (over y, x, core), row: 4 (over z).
Axes of the slice: x: 2, y: 2, z: 4, core: 2. Of those that a mesh axis runs over, the one named last changes fastest.
Arguments:
- starts: float32 [8, 8, 16384], P('tm', None, 'row'), may hold values from -6 to 6
- operator: float32 [16384, 16384], P('row', 'tm'), may hold values from -0.5 to 0.5
- coarse_left: float32 [16384, 256], P('row'), may hold values from -0.375 to 0.375
- coarse_right: float32 [16384, 256], P('row'), may hold values from -0.046875 to 0.046875
Outputs:
- new_ends: float32 [8, 8, 16384], P('tm', None, 'row')
The draws below stay inside these ranges and needn't reach their ends.
All inputs are finite; a program needn't handle non-finite values.
Results may differ from the reference program's by a relative error of at most 0.00019.
Values sent between devices are 32-bit elements; how exact they have to be, the bound alone decides.
A program may use at most 128 MiB of HBM per device.

```python
import jax
import jax.numpy as jnp
from jax import lax

N = 16384
R = 256
E = 8
FINE = 4
SLICES = 8


def shard_levels(stream_key, dims, pieces, smallest, largest):
    level, own = 1.0, jax.random.fold_in(stream_key, 6)
    for dim, shards_of in pieces:
        draws = jnp.exp(jax.random.uniform(jax.random.fold_in(own, dim), (shards_of,), jnp.float32, smallest / len(pieces), largest / len(pieces)))
        level = level * jnp.repeat(draws, dims[dim] // shards_of).reshape([-1 if axis == dim else 1 for axis in range(len(dims))])
    return level


def bell_draw(key, extent, deviation, most, split=(), dtype=jnp.bfloat16):
    values = jax.random.normal(key, extent, jnp.float32) * deviation
    if len(split) > 0:
        values = shard_levels(key, extent, split, -0.22, 0.18) * values
    return jnp.clip(values, min=-most, max=most).astype(dtype)


def setup_inputs(seed: int = 0) -> dict:
    keys = jax.random.split(jax.random.key(seed), 5)
    starts = bell_draw(keys[0], (SLICES, E, N), 1.0, 6.0, ((0, 8), (2, 4)), jnp.float32)
    operator = bell_draw(keys[1], (N, N), (max(1, 8 * N // (SLICES * FINE) ** 2)) ** -0.5, 0.5, ((0, 4), (1, 8)), jnp.float32)
    coarse_left = bell_draw(keys[2], (N, R), R ** -0.5, 0.375, ((0, 4),), jnp.float32)
    coarse_right = bell_draw(keys[3], (N, R), N ** -0.5, 0.046875, ((0, 4),), jnp.float32)
    return {"starts": starts, "operator": operator, "coarse_left": coarse_left, "coarse_right": coarse_right}


highest = lax.Precision.HIGHEST


def reference(starts, operator, coarse_left, coarse_right):
    slices = starts.shape[0]
    step_time = 1.0 / slices
    fine_time = step_time / FINE
    flattened = starts.reshape(slices * E, N)

    def fine_step(current, unused):
        images = lax.dot_general(current, operator, (((1,), (1,)), ((), ())), precision=highest, preferred_element_type=jnp.float32)
        return current + fine_time * images, None

    flattened, unused_out = lax.scan(fine_step, flattened, None, length=FINE)
    fine_ends = flattened.reshape(slices, E, N)
    old_projection = jnp.einsum("sen,nr->ser", starts, coarse_right, precision=highest)
    defects = fine_ends - (starts + step_time * jnp.einsum("ser,nr->sen", old_projection, coarse_left, precision=highest))

    def sweep_step(current, defect):
        projection = jnp.dot(current, coarse_right, precision=highest, preferred_element_type=jnp.float32)
        following = current + step_time * jnp.dot(projection, coarse_left.T, precision=highest, preferred_element_type=jnp.float32) + defect
        return following, following

    unused_last, new_ends = lax.scan(sweep_step, starts[0], defects)
    return new_ends
```

```python
import functools

import jax
import jax.numpy as jnp
from jax import lax
from jax.experimental import pallas as pl
from jax.experimental.pallas import tpu as pltpu
from jax.sharding import PartitionSpec as P

FINE = 4
MESH = pl.DeviceIdType.MESH

highest = lax.Precision.HIGHEST


def fine_kernel(
    T, R, fine_time,
    starts_ref, op_ref, first_ref, fine_ref,
    stage, pairs, arrivals, state, along, pieces, columns, half_send, half_recv, full_send, full_recv, own,
    load_sem, init_send, init_recv, z_send, z_recv, g_send, g_recv, h_send, h_recv, f_send, f_recv,
):
    t, r = lax.axis_index("tm"), lax.axis_index("row")
    E, rows = starts_ref.shape
    sub = rows // T
    S = T * E
    half = T // 2
    my_chip, my_core = t // 2, t % 2
    stage_rows = stage.shape[1]
    loads = rows // stage_rows

    def copy_to(src, dst, send, recv, tm, row):
        return pltpu.make_async_remote_copy(
            src_ref=src, dst_ref=dst, send_sem=send, recv_sem=recv, device_id=(tm, row), device_id_type=MESH
        )

    def load(k):
        slot = k % 2
        return pltpu.make_async_copy(
            op_ref.at[pl.ds(k * stage_rows, stage_rows)], stage.at[slot], load_sem.at[slot]
        )

    def init_copy(d):
        dest = lax.rem(t + d, T)
        src = starts_ref.at[:, pl.ds(pl.multiple_of(dest * sub, sub), sub)]
        return copy_to(src, arrivals.at[t], init_send.at[dest], init_recv.at[t], dest, r)

    for d in range(1, T):
        init_copy(d).start()
    load(0).start()
    load(1).start()

    def convert(k, unused):
        load(k).wait()
        base = pl.multiple_of(k * stage_rows, stage_rows)
        for c in range(R):
            x = stage[k % 2, :, c * sub : (c + 1) * sub]
            high = x.astype(jnp.bfloat16)
            low = (x - high.astype(jnp.float32)).astype(jnp.bfloat16)
            pairs[pl.ds(base, stage_rows), 2 * c * sub : (2 * c + 1) * sub] = high
            pairs[pl.ds(base, stage_rows), (2 * c + 1) * sub : (2 * c + 2) * sub] = low

        @pl.when(k + 2 < loads)
        def _():
            load(k + 2).start()

        return unused

    quarter = max(loads // 4, 1)
    bounds = [0, quarter, loads]

    lax.fori_loop(bounds[0], bounds[1], convert, 0)
    arrivals[t] = starts_ref[:, pl.ds(pl.multiple_of(t * sub, sub), sub)]
    for d in range(1, T):
        source = lax.rem(t + T - d, T)
        copy_to(arrivals.at[source], arrivals.at[source], init_send.at[source], init_recv.at[source], source, r).wait_recv()
    for k in range(T):
        state[k * E : (k + 1) * E, :] = arrivals[k]
        first_ref[k * E : (k + 1) * E, :] = arrivals[k]

    def step(i, filler):
        def z_copy(d):
            dest = lax.rem(r + d, R)
            return copy_to(state, along.at[i, r], z_send.at[dest], z_recv.at[i, r], t, dest)

        order = [d for d in range(1, R)]
        for d in order:
            z_copy(d).start()
        if filler is not None:
            filler()

        def piece_copy(source_row, block):
            index = source_row * T + t
            dest = index // R
            place = lax.rem(index, R)
            return dest, place, copy_to(
                block, pieces.at[i, place], g_send.at[source_row], g_recv.at[i, place], dest, r
            )

        def forward(source_row, block):
            dest, place, copy = piece_copy(source_row, block)

            @pl.when(dest != t)
            def _():
                copy.start()

            @pl.when(dest == t)
            def _():
                pieces[i, place] = block[...]

        forward(r, state)
        for d in order:
            source_row = lax.rem(r + R - d, R)
            copy_to(along.at[i, source_row], along.at[i, source_row], z_send.at[source_row], z_recv.at[i, source_row], t, source_row).wait_recv()
            forward(source_row, along.at[i, source_row])

        for j in range(R):
            source = lax.rem(t * R + j, T)

            @pl.when(source != t)
            def _():
                copy_to(pieces.at[i, j], pieces.at[i, j], g_send.at[j], g_recv.at[i, j], source, r).wait_recv()

            x = pieces[i, j]
            high = x.astype(jnp.bfloat16).astype(jnp.float32)
            both = jnp.concatenate([high, x - high], axis=0)
            turned = both.T.astype(jnp.bfloat16)
            columns[2 * j * sub : (2 * j + 1) * sub, :] = turned
            columns[(2 * j + 1) * sub : (2 * j + 2) * sub, :] = turned

        def image(target):
            base = pl.multiple_of(target * sub, sub)
            out = jnp.dot(pairs[pl.ds(base, sub), :], columns[...], preferred_element_type=jnp.float32)
            out = out.T
            return out[:S] + out[S:]

        def chip_at(k):
            return lax.rem(my_chip + 1 + k, half)

        def half_copy(q):
            return copy_to(half_send.at[q], half_recv.at[i, q], h_send.at[q], h_recv.at[i, q], t + 1 - 2 * my_core, r)

        def full_copy(q):
            return copy_to(full_send.at[q], full_recv.at[i, my_chip], f_send.at[q], f_recv.at[i, my_chip], 2 * q + my_core, r)

        def for_partner(k, unused):
            q = chip_at(k)
            half_send[q] = image(2 * q + 1 - my_core)
            half_copy(q).start()
            return unused

        lax.fori_loop(0, half, for_partner, 0)

        def for_others(k, unused):
            q = chip_at(k)
            mine = image(2 * q + my_core)
            half_copy(q).wait_recv()
            both = mine + half_recv[i, q]

            @pl.when(k < half - 1)
            def _():
                full_send[q] = both
                full_copy(q).start()

            @pl.when(k == half - 1)
            def _():
                own[...] = both

            return unused

        lax.fori_loop(0, half, for_others, 0)

        for d in order:
            z_copy(d).wait_send()
        for row in range(R):
            dest, unused_place, copy = piece_copy(jnp.int32(row), state)

            @pl.when(dest != t)
            def _():
                copy.wait_send()

        total = own[...]
        for k in range(half - 1):
            q = lax.rem(my_chip + half - 1 - k, half)
            copy_to(full_recv.at[i, q], full_recv.at[i, q], f_send.at[q], f_recv.at[i, q], 2 * q + my_core, r).wait_recv()
            total = total + full_recv[i, q]
        state[...] = state[...] + fine_time * total
        for q in range(half):
            half_copy(q).wait_send()

            @pl.when(q != my_chip)
            def _():
                full_copy(q).wait_send()

    def rest():
        lax.fori_loop(bounds[1], bounds[2], convert, 0)

    step(0, rest)
    for d in range(1, T):
        init_copy(d).wait_send()

    def later(i, unused):
        step(i, None)
        return unused

    lax.fori_loop(1, FINE, later, 0)
    fine_ref[...] = state[...]


def fine_steps(starts, operator, T, R, fine_time):
    E, rows = starts.shape
    columns = operator.shape[1]
    sub = rows // T
    S = T * E
    half = T // 2
    stage_rows = min(256, rows // 8)
    f32, bf16 = jnp.float32, jnp.bfloat16
    dma = pltpu.SemaphoreType.DMA
    vmem = pl.BlockSpec(memory_space=pltpu.VMEM)
    return pl.pallas_call(
        functools.partial(fine_kernel, T, R, fine_time),
        out_shape=[jax.ShapeDtypeStruct((S, sub), f32)] * 2,
        in_specs=[vmem, pl.BlockSpec(memory_space=pl.ANY)],
        out_specs=[vmem, vmem],
        scratch_shapes=[
            pltpu.VMEM((2, stage_rows, columns), f32),
            pltpu.VMEM((rows, 2 * columns), bf16),
            pltpu.VMEM((T, E, sub), f32),
            pltpu.VMEM((S, sub), f32),
            pltpu.VMEM((FINE, R, S, sub), f32),
            pltpu.VMEM((FINE, R, S, sub), f32),
            pltpu.VMEM((2 * columns, 2 * S), bf16),
            pltpu.VMEM((half, S, sub), f32),
            pltpu.VMEM((FINE, half, S, sub), f32),
            pltpu.VMEM((half, S, sub), f32),
            pltpu.VMEM((FINE, half, S, sub), f32),
            pltpu.VMEM((S, sub), f32),
            dma((2,)),
            dma((T,)),
            dma((T,)),
            dma((R,)),
            dma((FINE, R)),
            dma((R,)),
            dma((FINE, R)),
            dma((half,)),
            dma((FINE, half)),
            dma((half,)),
            dma((FINE, half)),
        ],
        compiler_params=pltpu.CompilerParams(has_side_effects=True, vmem_limit_bytes=60 * 2**20),
    )(starts, operator)


def local(starts, operator, coarse_left, coarse_right):
    T, R = lax.axis_size("tm"), lax.axis_size("row")
    t = lax.axis_index("tm")
    E, rows = starts.shape[1:]
    sub = rows // T
    rank = coarse_right.shape[1]
    step_time = 1.0 / T
    cross = lax.psum(jnp.dot(coarse_left.T, coarse_right, precision=highest), "row")
    first, fine = fine_steps(starts[0], operator, T, R, step_time / FINE)
    right = lax.dynamic_slice_in_dim(coarse_right, t * sub, sub, 0)
    both = jnp.concatenate([first, fine], axis=0)
    projected = lax.psum(jnp.dot(both, right, precision=highest), ("tm", "row"))
    old = projected[: T * E].reshape(T, E, rank)
    new = projected[T * E :].reshape(T, E, rank)
    first, fine = first.reshape(T, E, sub), fine.reshape(T, E, sub)
    sums = first[:1] + jnp.cumsum(fine - first, axis=0)
    sums = lax.all_to_all(sums, "tm", split_axis=0, concat_axis=2, tiled=True)
    kernel = jnp.eye(rank, dtype=jnp.float32) + step_time * cross
    w = jnp.zeros((E, rank), jnp.float32)
    total = w
    mine = w
    for m in range(T - 1):
        w = jnp.dot(w, kernel, precision=highest) + new[m] - old[m + 1]
        total = total + w
        mine = jnp.where(t == m + 1, total, mine)
    spread = lax.dot_general(mine, coarse_left, (((1,), (1,)), ((), ())), precision=highest)
    return sums + (step_time * spread)[None]


def solution(mesh):
    in_specs = (P("tm", None, "row"), P("row", "tm"), P("row", None), P("row", None))
    out_specs = P("tm", None, "row")
    return jax.shard_map(local, mesh=mesh, in_specs=in_specs, out_specs=out_specs, check_vma=False)
```

```python
import functools

import jax
import jax.numpy as jnp
from jax import lax
from jax.experimental import pallas as pl
from jax.experimental.pallas import tpu as pltpu
from jax.sharding import PartitionSpec as P

FINE = 4
MESH = pl.DeviceIdType.MESH

highest = lax.Precision.HIGHEST


def fine_kernel(
    T, R, fine_time,
    starts_ref, op_ref, first_ref, fine_ref,
    stage, pairs, arrivals, state, along, pieces, columns, half_send, half_recv, full_send, full_recv, own,
    load_sem, init_send, init_recv, z_send, z_recv, g_send, g_recv, h_send, h_recv, f_send, f_recv,
):
    t, r = lax.axis_index("tm"), lax.axis_index("row")
    E, rows = starts_ref.shape
    sub = rows // T
    S = T * E
    half = T // 2
    my_chip, my_core = t // 2, t % 2
    stage_rows = stage.shape[1]
    loads = rows // stage_rows

    def copy_to(src, dst, send, recv, tm, row):
        return pltpu.make_async_remote_copy(
            src_ref=src, dst_ref=dst, send_sem=send, recv_sem=recv, device_id=(tm, row), device_id_type=MESH
        )

    def load(k):
        slot = k % 2
        return pltpu.make_async_copy(
            op_ref.at[pl.ds(k * stage_rows, stage_rows)], stage.at[slot], load_sem.at[slot]
        )

    def init_copy(d):
        dest = lax.rem(t + d, T)
        src = starts_ref.at[:, pl.ds(pl.multiple_of(dest * sub, sub), sub)]
        return copy_to(src, arrivals.at[t], init_send.at[dest], init_recv.at[t], dest, r)

    for d in range(1, T):
        init_copy(d).start()
    load(0).start()
    load(1).start()

    def convert(k, unused):
        load(k).wait()
        base = pl.multiple_of(k * stage_rows, stage_rows)
        for c in range(R):
            x = stage[k % 2, :, c * sub : (c + 1) * sub]
            high = x.astype(jnp.bfloat16)
            low = (x - high.astype(jnp.float32)).astype(jnp.bfloat16)
            pairs[pl.ds(base, stage_rows), 2 * c * sub : (2 * c + 1) * sub] = high
            pairs[pl.ds(base, stage_rows), (2 * c + 1) * sub : (2 * c + 2) * sub] = low

        @pl.when(k + 2 < loads)
        def _():
            load(k + 2).start()

        return unused

    quarter = max(loads // 4, 1)
    bounds = [0, quarter, loads]

    lax.fori_loop(bounds[0], bounds[1], convert, 0)
    arrivals[t] = starts_ref[:, pl.ds(pl.multiple_of(t * sub, sub), sub)]
    for d in range(1, T):
        source = lax.rem(t + T - d, T)
        copy_to(arrivals.at[source], arrivals.at[source], init_send.at[source], init_recv.at[source], source, r).wait_recv()
    for k in range(T):
        state[k * E : (k + 1) * E, :] = arrivals[k]
        first_ref[k * E : (k + 1) * E, :] = arrivals[k]

    def step(i, filler):
        def z_copy(d):
            dest = lax.rem(r + d, R)
            return copy_to(state, along.at[i, r], z_send.at[dest], z_recv.at[i, r], t, dest)

        order = [d for d in range(1, R)]
        for d in order:
            z_copy(d).start()
        if filler is not None:
            filler()

        def piece_copy(source_row, block):
            index = source_row * T + t
            dest = index // R
            place = lax.rem(index, R)
            return dest, place, copy_to(
                block, pieces.at[i, place], g_send.at[source_row], g_recv.at[i, place], dest, r
            )

        def forward(source_row, block):
            dest, place, copy = piece_copy(source_row, block)

            @pl.when(dest != t)
            def _():
                copy.start()

            @pl.when(dest == t)
            def _():
                pieces[i, place] = block[...]

        forward(r, state)
        for d in order:
            source_row = lax.rem(r + R - d, R)
            copy_to(along.at[i, source_row], along.at[i, source_row], z_send.at[source_row], z_recv.at[i, source_row], t, source_row).wait_recv()
            forward(source_row, along.at[i, source_row])

        for j in range(R):
            source = lax.rem(t * R + j, T)

            @pl.when(source != t)
            def _():
                copy_to(pieces.at[i, j], pieces.at[i, j], g_send.at[j], g_recv.at[i, j], source, r).wait_recv()

            x = pieces[i, j]
            high = x.astype(jnp.bfloat16).astype(jnp.float32)
            both = jnp.concatenate([high, x - high], axis=0)
            turned = both.T.astype(jnp.bfloat16)
            columns[2 * j * sub : (2 * j + 1) * sub, :] = turned
            columns[(2 * j + 1) * sub : (2 * j + 2) * sub, :] = turned

        def image(target):
            base = pl.multiple_of(target * sub, sub)
            out = jnp.dot(pairs[pl.ds(base, sub), :], columns[...], preferred_element_type=jnp.float32)
            out = out.T
            return out[:S] + out[S:]

        def chip_at(k):
            return lax.rem(my_chip + 1 + k, half)

        def half_copy(q):
            return copy_to(half_send.at[q], half_recv.at[i, q], h_send.at[q], h_recv.at[i, q], t + 1 - 2 * my_core, r)

        def full_copy(q):
            return copy_to(full_send.at[q], full_recv.at[i, my_chip], f_send.at[q], f_recv.at[i, my_chip], 2 * q + my_core, r)

        def for_partner(k, unused):
            q = chip_at(k)
            half_send[q] = image(2 * q + 1 - my_core)
            half_copy(q).start()
            return unused

        lax.fori_loop(0, half, for_partner, 0)

        def for_others(k, unused):
            q = chip_at(k)
            mine = image(2 * q + my_core)
            half_copy(q).wait_recv()
            both = mine + half_recv[i, q]

            @pl.when(k < half - 1)
            def _():
                full_send[q] = both
                full_copy(q).start()

            @pl.when(k == half - 1)
            def _():
                own[...] = both

            return unused

        lax.fori_loop(0, half, for_others, 0)

        for d in order:
            z_copy(d).wait_send()
        for row in range(R):
            dest, unused_place, copy = piece_copy(jnp.int32(row), state)

            @pl.when(dest != t)
            def _():
                copy.wait_send()

        total = own[...]
        for k in range(half - 1):
            q = lax.rem(my_chip + half - 1 - k, half)
            copy_to(full_recv.at[i, q], full_recv.at[i, q], f_send.at[q], f_recv.at[i, q], 2 * q + my_core, r).wait_recv()
            total = total + full_recv[i, q]
        state[...] = state[...] + fine_time * total
        for q in range(half):
            half_copy(q).wait_send()

            @pl.when(q != my_chip)
            def _():
                full_copy(q).wait_send()

    def rest():
        lax.fori_loop(bounds[1], bounds[2], convert, 0)

    step(0, rest)
    for d in range(1, T):
        init_copy(d).wait_send()

    def later(i, unused):
        step(i, None)
        return unused

    lax.fori_loop(1, FINE, later, 0)
    fine_ref[...] = state[...]


def fine_steps(starts, operator, T, R, fine_time):
    E, rows = starts.shape
    columns = operator.shape[1]
    sub = rows // T
    S = T * E
    half = T // 2
    stage_rows = min(256, rows // 8)
    f32, bf16 = jnp.float32, jnp.bfloat16
    dma = pltpu.SemaphoreType.DMA
    vmem = pl.BlockSpec(memory_space=pltpu.VMEM)
    return pl.pallas_call(
        functools.partial(fine_kernel, T, R, fine_time),
        out_shape=[jax.ShapeDtypeStruct((S, sub), f32)] * 2,
        in_specs=[vmem, pl.BlockSpec(memory_space=pl.ANY)],
        out_specs=[vmem, vmem],
        scratch_shapes=[
            pltpu.VMEM((2, stage_rows, columns), f32),
            pltpu.VMEM((rows, 2 * columns), bf16),
            pltpu.VMEM((T, E, sub), f32),
            pltpu.VMEM((S, sub), f32),
            pltpu.VMEM((FINE, R, S, sub), f32),
            pltpu.VMEM((FINE, R, S, sub), f32),
            pltpu.VMEM((2 * columns, 2 * S), bf16),
            pltpu.VMEM((half, S, sub), f32),
            pltpu.VMEM((FINE, half, S, sub), f32),
            pltpu.VMEM((half, S, sub), f32),
            pltpu.VMEM((FINE, half, S, sub), f32),
            pltpu.VMEM((S, sub), f32),
            dma((2,)),
            dma((T,)),
            dma((T,)),
            dma((R,)),
            dma((FINE, R)),
            dma((R,)),
            dma((FINE, R)),
            dma((half,)),
            dma((FINE, half)),
            dma((half,)),
            dma((FINE, half)),
        ],
        compiler_params=pltpu.CompilerParams(has_side_effects=True, vmem_limit_bytes=60 * 2**20),
    )(starts, operator)


def local(starts, operator, coarse_left, coarse_right):
    T, R = lax.axis_size("tm"), lax.axis_size("row")
    t = lax.axis_index("tm")
    E, rows = starts.shape[1:]
    sub = rows // T
    rank = coarse_right.shape[1]
    step_time = 1.0 / T
    first, fine = fine_steps(starts[0], operator, T, R, step_time / FINE)
    right = lax.dynamic_slice_in_dim(coarse_right, t * sub, sub, 0)
    both = jnp.concatenate([first, fine], axis=0)
    width = rank // T
    left = lax.dynamic_slice_in_dim(coarse_left, t * width, width, 1)
    cross_part = lax.dot_general(left, coarse_right, (((0,), (0,)), ((), ())), precision=highest)
    part = jnp.dot(both, right, precision=highest).reshape(T, 2 * E, rank)
    part = jnp.sum(lax.all_to_all(part, "tm", split_axis=0, concat_axis=0, tiled=True), axis=0)
    part = jnp.sum(lax.all_gather(jnp.concatenate([part, cross_part], axis=0), "row"), axis=0)
    parts = lax.all_gather(part, "tm")
    projected = parts[:, : 2 * E].reshape(2 * T * E, rank)
    cross = parts[:, 2 * E :].reshape(rank, rank)
    old = projected[: T * E].reshape(T, E, rank)
    new = projected[T * E :].reshape(T, E, rank)
    first, fine = first.reshape(T, E, sub), fine.reshape(T, E, sub)
    sums = first[:1] + jnp.cumsum(fine - first, axis=0)
    sums = lax.all_to_all(sums, "tm", split_axis=0, concat_axis=2, tiled=True)
    kernel = jnp.eye(rank, dtype=jnp.float32) + step_time * cross
    w = jnp.zeros((E, rank), jnp.float32)
    total = w
    mine = w
    for m in range(T - 1):
        w = jnp.dot(w, kernel, precision=highest) + new[m] - old[m + 1]
        total = total + w
        mine = jnp.where(t == m + 1, total, mine)
    spread = lax.dot_general(mine, coarse_left, (((1,), (1,)), ((), ())), precision=highest)
    return sums + (step_time * spread)[None]


def solution(mesh):
    in_specs = (P("tm", None, "row"), P("row", "tm"), P("row", None), P("row", None))
    out_specs = P("tm", None, "row")
    return jax.shard_map(local, mesh=mesh, in_specs=in_specs, out_specs=out_specs, check_vma=False)
```
